768 devices in a mesh: dp: 96 (over z_lo, y, x), tp: 8 (over z_hi, core).
Axes of the slice: x: 4, y: 8, z: 12 (z_hi: 4, z_lo: 3; z = z_hi * 3 + z_lo), core: 2. Of those that a mesh axis runs over, the one named last changes fastest.
Arguments:
- resid: bfloat16 [24576, 4096], P('dp'), may hold values from -6 to 6
- gain: bfloat16 [4096], replicated, may hold values from 0.25 to 1.75
- grad_q: bfloat16 [24576, 3072], P('dp', 'tp'), may hold values from -3 to 3
- w_query: bfloat16 [3072, 4096], P('tp'), may hold values from -0.375 to 0.375
- grad_in: bfloat16 [24576, 4096], P('dp'), may hold values from -2 to 2
Outputs:
- weight_grad: float32 [3072, 4096], P(('tp', 'dp'))
- gain_grad: float32 [4096], replicated
- grad_out: bfloat16 [24576, 4096], P('dp')
The draws below stay inside these ranges and needn't reach their ends.
All inputs are finite; a program needn't handle non-finite values.
Results may differ from the reference program's by a relative error of at most 0.014.
Values may be sent and summed in bfloat16 or wider, within the bound.
No kernel may reach another device: no remote copies, remote signals or barrier semaphores. Data moves between devices by JAX's collectives and lax.ppermute only.
A program may use at most 64 MiB of HBM per device.

```python
import jax
import jax.numpy as jnp
from jax import lax

D = 4096
QW = 3072
TOKENS = 24576
N_TP = 8


def with_spikes(drawn, stream_key, source, target, parts, factor):
    owner, partner = [(jnp.arange(drawn.shape[dim]) // (drawn.shape[dim] // parts)).reshape([-1 if axis == dim else 1 for axis in range(drawn.ndim)]) for dim in (source, target)]
    chosen = jax.random.permutation(stream_key, parts)[partner]
    strong = (owner == chosen) | (owner == (partner + parts // 2) % parts)
    return jnp.where(strong, factor * drawn, drawn)


def shard_levels(key, dims, cuts, low, top_value):
    def one(dim, parts):
        draws = jax.random.uniform(jax.random.fold_in(jax.random.fold_in(key, 6), dim), (parts,), jnp.float32, low / len(cuts), top_value / len(cuts))
        return jnp.repeat(jnp.exp(draws), dims[dim] // parts).reshape((-1,) + (1,) * (len(dims) - dim - 1))

    level = one(*cuts[0])
    for cut in cuts[1:]:
        level = level * one(*cut)
    return level


def gaussian(own_key, extent, scale, bound, split=(), dtype=jnp.bfloat16):
    drawn = scale * jax.random.normal(own_key, extent, jnp.float32)
    if split:
        drawn = drawn * shard_levels(own_key, extent, split, -0.22, 0.18)
    return jnp.clip(drawn, -bound, bound).astype(dtype)


def gaussian_with(stream_key, dims, deviation, reach, split, heavy, kind=jnp.bfloat16):
    values = deviation * jax.random.normal(stream_key, dims, jnp.float32)
    if split:
        values = values * shard_levels(stream_key, dims, split, -0.22, 0.18)
    return jnp.clip(with_spikes(values, jax.random.fold_in(stream_key, 3), *heavy), -reach, reach).astype(kind)


def setup_inputs(seed: int = 0) -> dict:
    streams_of = jax.random.split(jax.random.key(seed), 6)
    resid = gaussian(streams_of[0], (TOKENS, D), 1.0, 6.0, ((0, 96),))
    gain = jnp.clip(1.0 + 0.15 * jax.random.normal(streams_of[1], (D,), jnp.float32), 0.25, 1.75).astype(jnp.bfloat16)
    grad_q = gaussian_with(streams_of[2], (TOKENS, QW), 0.0625, 3.0, ((0, 96), (1, 8)), (0, 1, 96, 4.75))
    w_query = gaussian(streams_of[3], (QW, D), (D // 16) ** -0.5, 0.375, ((0, 8),))
    grad_in = gaussian(streams_of[4], (TOKENS, D), 0.125, 2.0, ((0, 96),))
    return dict(resid=resid, gain=gain, grad_q=grad_q, w_query=w_query, grad_in=grad_in)


def reference(resid, gain, grad_q, w_query, grad_in):
    resid_f = resid.astype(jnp.float32)
    gain_f = gain.astype(jnp.float32)
    inv_rms = lax.rsqrt(lax.optimization_barrier(jnp.mean(resid_f * resid_f, axis=-1, keepdims=True)) + 1e-05)
    unit = resid_f * inv_rms
    normed = (unit * gain_f).astype(jnp.bfloat16)
    weight_grad = jnp.dot(grad_q.astype(jnp.float32).T, normed.astype(jnp.float32), preferred_element_type=jnp.float32)
    block = QW // N_TP
    dnormed = jnp.zeros(resid.shape, jnp.float32)
    for index in range(N_TP):
        cols = grad_q[:, index * block:(index + 1) * block].astype(jnp.float32)
        rows = w_query[index * block:(index + 1) * block, :].astype(jnp.float32)
        partial_value = jnp.dot(cols, rows, preferred_element_type=jnp.float32).astype(jnp.bfloat16)
        dnormed = dnormed + partial_value.astype(jnp.float32)
    gain_grad = lax.optimization_barrier(jnp.sum(dnormed * unit, axis=0))
    dunit = dnormed * gain_f
    inner = lax.optimization_barrier(jnp.mean(dunit * unit, axis=-1, keepdims=True))
    grad_out = (grad_in.astype(jnp.float32) + inv_rms * (dunit - unit * inner)).astype(jnp.bfloat16)
    return (weight_grad, gain_grad, grad_out)
```

```python
import jax
import jax.numpy as jnp
from jax import lax
from jax.sharding import Mesh
from jax.sharding import PartitionSpec as P

DP = ("zl", "y", "x")
TP = ("zh", "c")
F32 = jnp.float32
BF16 = jnp.bfloat16


def exchange(blocks, axes):
    return lax.all_to_all(blocks, axes, 0, 0, tiled=True)


def spread(block, axes):
    peers = lax.axis_size(axes)
    return exchange(jnp.broadcast_to(block[None], (peers, *block.shape)), axes)


def total(blocks):
    return jnp.sum(blocks.astype(F32), axis=0)


def shifted(block, axis, shift):
    peers = lax.axis_size(axis)
    return lax.ppermute(block, axis, [(i, (i + shift) % peers) for i in range(peers)])


def owner_major(cols):
    zl, y, x = (lax.axis_size(a) for a in DP)
    rows = cols // (zl * y * x)
    place = jnp.arange(cols)
    owner, row = place // rows % (zl * y), place % rows
    source = owner * (x * rows) + place // (zl * y * rows) * rows + row
    return (place[:, None] == source[None, :]).astype(BF16)


def body(resid, gain, grad_q, w_query, grad_in):
    tokens, width = resid.shape
    cols = grad_q.shape[1]
    core, zh = lax.axis_index("c"), lax.axis_index("zh")
    n_zh, n_x, n_y, n_zl = (lax.axis_size(a) for a in ("zh", "x", "y", "zl"))
    half = tokens // 2
    own = half // n_zh
    swap = [(0, 1), (1, 0)]
    gain_f = gain.astype(F32)

    def rows_of(array, start, size):
        return lax.dynamic_slice_in_dim(array, start, size, 0)

    def norm(rows):
        rows_f = rows.astype(F32)
        inv = lax.rsqrt(jnp.mean(rows_f * rows_f, axis=-1, keepdims=True) + 1e-05)
        return inv, rows_f * inv

    def term(start):
        return jnp.dot(rows_of(grad_q, start, half), w_query, preferred_element_type=F32)

    other_start, own_start = (1 - core) * half, core * half
    sent = term(other_start)
    got = lax.ppermute(sent.astype(BF16), "c", swap)
    kept = term(own_start)
    pair = (kept + got.astype(F32)).astype(BF16)

    _, unit = norm(resid)
    unit_other, unit_own = rows_of(unit, other_start, half), rows_of(unit, own_start, half)
    part = jnp.sum(sent * unit_other, axis=0) + jnp.sum(kept * unit_own, axis=0)
    part = total(spread(part.reshape(-1, 128), TP)).reshape(-1)

    dnormed = rows_of(pair, zh * own, own).astype(F32)
    for shift in range(1, n_zh):
        block = rows_of(pair, lax.rem(zh + shift, n_zh) * own, own)
        dnormed = dnormed + shifted(block, "zh", shift).astype(F32)

    normed = (unit * gain_f).astype(BF16)
    ordered = jnp.dot(grad_q, owner_major(cols), preferred_element_type=F32).astype(BF16)
    local = lax.dot_general(
        ordered, normed, (((0,), (0,)), ((), ())), preferred_element_type=F32
    ).astype(BF16)
    upper = part.astype(BF16)
    lower = (part - upper.astype(F32)).astype(BF16)
    rider = jnp.pad(jnp.stack([upper, lower]), ((0, 6), (0, 0)))
    share = cols // n_x
    rider = jnp.broadcast_to(rider[None], (n_x, 8, width))
    by_x = total(exchange(jnp.concatenate([local.reshape(n_x, share, width), rider], axis=1), "x"))
    part = by_x[share] + by_x[share + 1]
    mine = share // (n_y * n_zl)
    by_x = by_x[:share].astype(BF16).reshape(n_zl * n_y, mine, width)
    rider = part.astype(BF16).reshape(1, mine, width // mine)
    rider = jnp.broadcast_to(rider, (n_zl * n_y, mine, width // mine))
    summed = total(exchange(jnp.concatenate([by_x, rider], axis=2), ("zl", "y")))
    weight_grad = summed[:, :width]
    gain_grad = summed[:, width:].reshape(-1)

    first = own_start + zh * own
    inv_own, unit_rows = norm(rows_of(resid, first, own))
    dunit = dnormed * gain_f
    inner = jnp.mean(dunit * unit_rows, axis=-1, keepdims=True)
    rows = rows_of(grad_in, first, own).astype(F32) + inv_own * (dunit - unit_rows * inner)
    rows = rows.astype(BF16)
    mine_half = lax.dynamic_update_slice_in_dim(jnp.zeros((half, width), BF16), rows, zh * own, 0)
    for shift in range(1, n_zh):
        source = lax.rem(zh + n_zh - shift, n_zh) * own
        mine_half = lax.dynamic_update_slice_in_dim(
            mine_half, shifted(rows, "zh", shift), source, 0
        )
    other_half = lax.ppermute(mine_half, "c", swap)
    low = jnp.where(core == 0, mine_half, other_half)
    high = jnp.where(core == 0, other_half, mine_half)
    return weight_grad, gain_grad, jnp.concatenate([low, high], axis=0)


def solution(mesh):
    finer = Mesh(mesh.devices.reshape(3, 8, 4, 4, 2), ("zl", "y", "x", "zh", "c"))
    in_specs = (P(DP, None), P(), P(DP, TP), P(TP, None), P(DP, None))
    out_specs = (P(TP + DP, None), P(), P(DP, None))
    return jax.shard_map(body, mesh=finer, in_specs=in_specs, out_specs=out_specs, check_vma=False)
```

```python
import jax
import jax.numpy as jnp
from jax import lax
from jax.sharding import Mesh
from jax.sharding import PartitionSpec as P


DP = ("zl", "y", "x")
TP = ("zh", "c")
F32 = jnp.float32
BF16 = jnp.bfloat16


def exchange(blocks, axes):
    return lax.all_to_all(blocks, axes, 0, 0, tiled=True)


def total(blocks):
    return jnp.sum(blocks.astype(F32), axis=0)


def shifted(block, axis, shift):
    peers = lax.axis_size(axis)
    return lax.ppermute(block, axis, [(i, (i + shift) % peers) for i in range(peers)])


def swapped(block, axis, bit):
    return lax.ppermute(block, axis, [(i, i ^ bit) for i in range(lax.axis_size(axis))])


def owner_columns(cols, x_index):
    zl, y, x = (lax.axis_size(a) for a in DP)
    rows = cols // (zl * y * x)
    place = jnp.arange(cols)
    shift, owner, row = place // (zl * y * rows), place // rows % (zl * y), place % rows
    source = owner * (x * rows) + lax.rem(shift + x_index, x) * rows + row
    return (place[:, None] == source[None, :]).astype(BF16)


def body(resid, gain, grad_q, w_query, grad_in):
    tokens, width = resid.shape
    cols = grad_q.shape[1]
    core, zh = lax.axis_index("c"), lax.axis_index("zh")
    n_zh, n_x, n_y, n_zl = (lax.axis_size(a) for a in ("zh", "x", "y", "zl"))
    half = tokens // 2
    own = half // n_zh
    gain_f = gain.astype(F32)

    def rows_of(array, start, size):
        return lax.dynamic_slice_in_dim(array, start, size, 0)

    def inverse(rows):
        rows_f = rows.astype(F32)
        return lax.rsqrt(jnp.mean(rows_f * rows_f, axis=-1, keepdims=True) + 1e-05)

    def term(start):
        return jnp.dot(rows_of(grad_q, start, half), w_query, preferred_element_type=F32)

    other_start, own_start = (1 - core) * half, core * half
    sent = term(other_start)
    got = swapped(sent.astype(BF16), "c", 1)
    kept = lax.optimization_barrier(term(own_start))
    pair = (kept + got.astype(F32)).astype(BF16)
    inv = inverse(resid)
    pair, inv = lax.optimization_barrier((pair, inv))
    dnormed = total(exchange(pair.reshape(n_zh, own, width), "zh"))

    unit = resid.astype(F32) * inv
    normed = (unit * gain_f).astype(BF16)
    ordered = jnp.dot(grad_q, owner_columns(cols, lax.axis_index("x")), preferred_element_type=F32)
    ordered = lax.optimization_barrier(ordered.astype(BF16))
    share = cols // n_x

    def block(shift):
        columns = ordered[:, shift * share : (shift + 1) * share]
        return lax.dot_general(
            columns, normed, (((0,), (0,)), ((), ())), preferred_element_type=F32
        )

    blocks = [block(s).astype(BF16) for s in range(1, n_x)]
    inv, *blocks = lax.optimization_barrier((inv, *blocks))
    by_x = [shifted(b, "x", s + 1) for s, b in enumerate(blocks)]
    unit = resid.astype(F32) * inv
    part = jnp.sum(sent * rows_of(unit, other_start, half), axis=0)
    part = part + jnp.sum(kept * rows_of(unit, own_start, half), axis=0)
    part = part.reshape(n_y, -1, 128)
    for bit in (1, 2, 4):
        part = part + swapped(part, "y", bit)
    part = lax.dynamic_index_in_dim(part, lax.axis_index("y"), 0, keepdims=False)
    axes = ("x", "zh", "c")
    part, dnormed = lax.optimization_barrier((part, dnormed))
    part = jnp.broadcast_to(part[None], (lax.axis_size(axes), *part.shape))
    part = total(exchange(part, axes))

    first = own_start + zh * own
    resid_rows = rows_of(resid, first, own)
    inv_rows = inverse(resid_rows)
    unit_rows = resid_rows.astype(F32) * inv_rows
    dunit = dnormed * gain_f
    inner = jnp.mean(dunit * unit_rows, axis=-1, keepdims=True)
    rows = rows_of(grad_in, first, own).astype(F32) + inv_rows * (dunit - unit_rows * inner)
    first_block, rows = lax.optimization_barrier((block(0), rows.astype(BF16)))

    by_x = first_block + sum(b.astype(F32) for b in by_x)
    mine = share // (n_y * n_zl)
    by_x = by_x.astype(BF16).reshape(n_zl * n_y, mine, width)

    upper = part.astype(BF16)
    lower = (part - upper.astype(F32)).astype(BF16)
    rider = jnp.concatenate([upper, lower], axis=1)
    rider = jnp.broadcast_to(rider[None], (n_zl * n_y, *rider.shape))
    last = exchange(jnp.concatenate([by_x, rider], axis=2), ("zl", "y"))
    weight_grad = total(last[:, :, :width])
    parts = last[:, :, width:].astype(F32)
    parts = (parts[:, :, :128] + parts[:, :, 128:]).reshape(n_zl, n_y, -1, 128)
    gain_grad = jnp.sum(parts, axis=0).reshape(-1)

    result = jnp.zeros((tokens, width), BF16)
    for shift in range(n_zh):
        piece = rows if shift == 0 else shifted(rows, "zh", shift)
        source = lax.rem(zh + n_zh - shift, n_zh) * own
        result = lax.dynamic_update_slice_in_dim(result, piece, own_start + source, 0)
        piece = swapped(piece, "c", 1)
        result = lax.dynamic_update_slice_in_dim(result, piece, other_start + source, 0)
    return weight_grad, gain_grad, result


def solution(mesh):
    finer = Mesh(mesh.devices.reshape(3, 8, 4, 4, 2), ("zl", "y", "x", "zh", "c"))
    in_specs = (P(DP, None), P(), P(DP, TP), P(TP, None), P(DP, None))
    out_specs = (P(TP + DP, None), P(), P(DP, None))
    return jax.shard_map(body, mesh=finer, in_specs=in_specs, out_specs=out_specs, check_vma=False)
```

```python
import jax
import jax.numpy as jnp
from jax import lax
from jax.sharding import Mesh
from jax.sharding import PartitionSpec as P


DP = ("zl", "y", "x")
TP = ("zh", "c")
F32 = jnp.float32
BF16 = jnp.bfloat16


def exchange(blocks, axes):
    return lax.all_to_all(blocks, axes, 0, 0, tiled=True)


def total(blocks):
    return jnp.sum(blocks.astype(F32), axis=0)


def shifted(block, axis, shift):
    peers = lax.axis_size(axis)
    return lax.ppermute(block, axis, [(i, (i + shift) % peers) for i in range(peers)])


def swapped(block, axis, bit):
    return lax.ppermute(block, axis, [(i, i ^ bit) for i in range(lax.axis_size(axis))])


def owner_columns(cols, x_index):
    zl, y, x = (lax.axis_size(a) for a in DP)
    rows = cols // (zl * y * x)
    place = jnp.arange(cols)
    shift, owner, row = place // (zl * y * rows), place // rows % (zl * y), place % rows
    source = owner * (x * rows) + lax.rem(shift + x_index, x) * rows + row
    return (place[:, None] == source[None, :]).astype(BF16)


def body(resid, gain, grad_q, w_query, grad_in):
    tokens, width = resid.shape
    cols = grad_q.shape[1]
    core, zh = lax.axis_index("c"), lax.axis_index("zh")
    n_zh, n_x, n_y, n_zl = (lax.axis_size(a) for a in ("zh", "x", "y", "zl"))
    half = tokens // 2
    own = half // n_zh
    gain_f = gain.astype(F32)

    def rows_of(array, start, size):
        return lax.dynamic_slice_in_dim(array, start, size, 0)

    def inverse(rows):
        rows_f = rows.astype(F32)
        return lax.rsqrt(jnp.mean(rows_f * rows_f, axis=-1, keepdims=True) + 1e-05)

    def term(start):
        rows = rows_of(grad_q, start, half)
        return jnp.dot(rows, w_query, preferred_element_type=F32).astype(BF16)

    inv = inverse(resid)
    ordered = jnp.dot(grad_q, owner_columns(cols, lax.axis_index("x")), preferred_element_type=F32)
    inv, ordered, grad_q = lax.optimization_barrier((inv, ordered.astype(BF16), grad_q))

    other_start, own_start = (1 - core) * half, core * half
    sent = term(other_start)
    got = swapped(sent, "c", 1)
    kept = lax.optimization_barrier(term(own_start))
    pair = (kept.astype(F32) + got.astype(F32)).astype(BF16)
    pair, inv = lax.optimization_barrier((pair, inv))
    dnormed = total(exchange(pair.reshape(n_zh, own, width), "zh"))

    unit = resid.astype(F32) * inv
    normed = (unit * gain_f).astype(BF16)
    share = cols // n_x

    def columns(shift):
        return ordered[:, shift * share : (shift + 1) * share]

    def block(columns):
        return lax.dot_general(
            columns, normed, (((0,), (0,)), ((), ())), preferred_element_type=F32
        )

    blocks = [block(columns(s)).astype(BF16) for s in range(1, n_x)]
    inv, *blocks = lax.optimization_barrier((inv, *blocks))
    by_x = [shifted(b, "x", s + 1) for s, b in enumerate(blocks)]
    unit = resid.astype(F32) * inv
    part = jnp.sum(sent.astype(F32) * rows_of(unit, other_start, half), axis=0)
    part = part + jnp.sum(kept.astype(F32) * rows_of(unit, own_start, half), axis=0)
    part = part.reshape(n_y, -1, 128)
    for bit in (1, 2, 4):
        part = part + swapped(part, "y", bit)
    part = lax.dynamic_index_in_dim(part, lax.axis_index("y"), 0, keepdims=False)
    axes = ("x", "zh", "c")
    part, dnormed = lax.optimization_barrier((part, dnormed))
    part = jnp.broadcast_to(part[None], (lax.axis_size(axes), *part.shape))
    part = total(exchange(part, axes))

    first = own_start + zh * own
    resid_rows = rows_of(resid, first, own)
    inv_rows = rows_of(inv, first, own)
    unit_rows = resid_rows.astype(F32) * inv_rows
    dunit = dnormed * gain_f
    inner = jnp.mean(dunit * unit_rows, axis=-1, keepdims=True)
    rows = rows_of(grad_in, first, own).astype(F32) + inv_rows * (dunit - unit_rows * inner)
    own_columns, rows = lax.optimization_barrier((columns(0), rows.astype(BF16)))

    by_x = block(own_columns) + sum(b.astype(F32) for b in by_x)
    mine = share // (n_y * n_zl)
    by_x = by_x.astype(BF16).reshape(n_zl * n_y, mine, width)

    upper = part.astype(BF16)
    lower = (part - upper.astype(F32)).astype(BF16)
    rider = jnp.concatenate([upper, lower], axis=1)
    rider = jnp.broadcast_to(rider[None], (n_zl * n_y, *rider.shape))
    last = exchange(jnp.concatenate([by_x, rider], axis=2), ("zl", "y"))
    weight_grad = total(last[:, :, :width])
    parts = last[:, :, width:].astype(F32)
    parts = (parts[:, :, :128] + parts[:, :, 128:]).reshape(n_zl, n_y, -1, 128)
    gain_grad = jnp.sum(parts, axis=0).reshape(-1)

    result = jnp.zeros((tokens, width), BF16)
    for shift in (0, 1, n_zh - 1, 2):
        piece = rows if shift == 0 else shifted(rows, "zh", shift)
        other = swapped(piece, "c", 1)
        source = lax.rem(zh + n_zh - shift, n_zh) * own
        result = lax.dynamic_update_slice_in_dim(result, piece, own_start + source, 0)
        result = lax.dynamic_update_slice_in_dim(result, other, other_start + source, 0)
    return weight_grad, gain_grad, result


def solution(mesh):
    finer = Mesh(mesh.devices.reshape(3, 8, 4, 4, 2), ("zl", "y", "x", "zh", "c"))
    in_specs = (P(DP, None), P(), P(DP, TP), P(TP, None), P(DP, None))
    out_specs = (P(TP + DP, None), P(), P(DP, None))
    return jax.shard_map(body, mesh=finer, in_specs=in_specs, out_specs=out_specs, check_vma=False)
```

```python
import jax
import jax.numpy as jnp
from jax import lax
from jax.experimental import pallas as pl
from jax.experimental.pallas import tpu as pltpu
from jax.sharding import Mesh
from jax.sharding import PartitionSpec as P


DP = ("zl", "y", "x")
TP = ("zh", "c")
F32 = jnp.float32
BF16 = jnp.bfloat16


def exchange(blocks, axes):
    return lax.all_to_all(blocks, axes, 0, 0, tiled=True)


def total(blocks):
    return jnp.sum(blocks.astype(F32), axis=0)


def shifted(block, axis, shift):
    peers = lax.axis_size(axis)
    return lax.ppermute(block, axis, [(i, (i + shift) % peers) for i in range(peers)])


def swapped(block, axis, bit):
    return lax.ppermute(block, axis, [(i, i ^ bit) for i in range(lax.axis_size(axis))])


def owner_columns(cols, x_index):
    zl, y, x = (lax.axis_size(a) for a in DP)
    rows = cols // (zl * y * x)
    place = jnp.arange(cols)
    shift, owner, row = place // (zl * y * rows), place // rows % (zl * y), place % rows
    source = owner * (x * rows) + lax.rem(shift + x_index, x) * rows + row
    return (place[:, None] == source[None, :]).astype(BF16)


def pack_kernel(first, second, third, fourth, rider, packed):
    owners, rows, _ = packed.shape
    width = first.shape[1]
    per_tile = 8 // rows
    for tile in range(owners // per_tile):
        place = slice(tile * 8, tile * 8 + 8)
        parts = [ref[place, :].astype(F32) for ref in (first, second, third, fourth)]
        summed = (parts[0] + parts[1]) + (parts[2] + parts[3])
        for one in range(per_tile):
            owner = tile * per_tile + one
            packed[owner, :, :width] = summed[one * rows : (one + 1) * rows, :].astype(BF16)
            packed[owner, :, width:] = rider[...]


def pack(blocks, rider):
    share, width = blocks[0].shape
    rows, extra = rider.shape
    shape = (share // rows, rows, width + extra)
    return pl.pallas_call(
        pack_kernel,
        out_shape=jax.ShapeDtypeStruct(shape, BF16),
        in_specs=[pl.BlockSpec(memory_space=pltpu.VMEM)] * 5,
        out_specs=pl.BlockSpec(memory_space=pltpu.VMEM),
        compiler_params=pltpu.CompilerParams(vmem_limit_bytes=10 * 2**20),
        cost_estimate=pl.CostEstimate(
            flops=3 * share * width, bytes_accessed=10 * share * width, transcendentals=0
        ),
        name="pack",
    )(*blocks, rider)


def body(resid, gain, grad_q, w_query, grad_in):
    tokens, width = resid.shape
    cols = grad_q.shape[1]
    core, zh = lax.axis_index("c"), lax.axis_index("zh")
    n_zh, n_x, n_y, n_zl = (lax.axis_size(a) for a in ("zh", "x", "y", "zl"))
    half = tokens // 2
    own = half // n_zh
    gain_f = gain.astype(F32)

    def rows_of(array, start, size):
        return lax.dynamic_slice_in_dim(array, start, size, 0)

    def inverse(rows):
        rows_f = rows.astype(F32)
        return lax.rsqrt(jnp.mean(rows_f * rows_f, axis=-1, keepdims=True) + 1e-05)

    def term(start):
        rows = rows_of(grad_q, start, half)
        return jnp.dot(rows, w_query, preferred_element_type=F32).astype(BF16)

    inv, grad_q = lax.optimization_barrier((inverse(resid), grad_q))
    ordered = jnp.dot(grad_q, owner_columns(cols, lax.axis_index("x")), preferred_element_type=F32)
    ordered = ordered.astype(BF16)

    other_start, own_start = (1 - core) * half, core * half
    sent = term(other_start)
    got = swapped(sent, "c", 1)
    kept = lax.optimization_barrier(term(own_start))
    pair = (kept.astype(F32) + got.astype(F32)).astype(BF16)
    pair, inv, ordered = lax.optimization_barrier((pair, inv, ordered))
    dnormed = total(exchange(pair.reshape(n_zh, own, width), "zh"))

    unit = resid.astype(F32) * inv
    part = jnp.sum(sent.astype(F32) * rows_of(unit, other_start, half), axis=0)
    part = part + jnp.sum(kept.astype(F32) * rows_of(unit, own_start, half), axis=0)
    part, inv_x = lax.optimization_barrier((part.reshape(n_y, -1, 128), inv))
    part = part + swapped(part, "y", 1)

    normed = (resid.astype(F32) * inv_x * gain_f).astype(BF16)
    share = cols // n_x

    def block(shift):
        columns = ordered[:, shift * share : (shift + 1) * share]
        local = lax.dot_general(
            columns, normed, (((0,), (0,)), ((), ())), preferred_element_type=F32
        )
        return lax.optimization_barrier(local.astype(BF16))

    blocks = [block(s) for s in range(n_x)]
    blocks = [b if s == 0 else shifted(b, "x", s) for s, b in enumerate(blocks)]
    for bit in (2, 4):
        part = part + swapped(part, "y", bit)
    part = lax.dynamic_index_in_dim(part, lax.axis_index("y"), 0, keepdims=False)

    first = own_start + zh * own
    resid_rows = rows_of(resid, first, own)
    inv_rows = rows_of(inv, first, own)
    unit_rows = resid_rows.astype(F32) * inv_rows
    dunit = dnormed * gain_f
    inner = jnp.mean(dunit * unit_rows, axis=-1, keepdims=True)
    axes = ("x", "zh", "c")
    part, inner = lax.optimization_barrier((part, inner))
    part = jnp.broadcast_to(part[None], (lax.axis_size(axes), *part.shape))
    part = total(exchange(part, axes))
    rows = rows_of(grad_in, first, own).astype(F32) + inv_rows * (dunit - unit_rows * inner)
    own_block, rows = lax.optimization_barrier((blocks[0], rows.astype(BF16)))

    upper = part.astype(BF16)
    lower = (part - upper.astype(F32)).astype(BF16)
    packed = pack([own_block, *blocks[1:]], jnp.concatenate([upper, lower], axis=1))
    last = exchange(packed, ("zl", "y"))
    weight_grad = total(last[:, :, :width])
    parts = last[:, :, width:].astype(F32)
    parts = (parts[:, :, :128] + parts[:, :, 128:]).reshape(n_zl, n_y, -1, 128)
    gain_grad = jnp.sum(parts, axis=0).reshape(-1)

    result = jnp.zeros((tokens, width), BF16)
    for shift in (0, 1, n_zh - 1, 2):
        piece = rows if shift == 0 else shifted(rows, "zh", shift)
        other = swapped(piece, "c", 1)
        source = lax.rem(zh + n_zh - shift, n_zh) * own
        result = lax.dynamic_update_slice_in_dim(result, piece, own_start + source, 0)
        result = lax.dynamic_update_slice_in_dim(result, other, other_start + source, 0)
    return weight_grad, gain_grad, result


def solution(mesh):
    finer = Mesh(mesh.devices.reshape(3, 8, 4, 4, 2), ("zl", "y", "x", "zh", "c"))
    in_specs = (P(DP, None), P(), P(DP, TP), P(TP, None), P(DP, None))
    out_specs = (P(TP + DP, None), P(), P(DP, None))
    return jax.shard_map(body, mesh=finer, in_specs=in_specs, out_specs=out_specs, check_vma=False)
```

```python
import jax
import jax.numpy as jnp
from jax import lax
from jax.experimental import pallas as pl
from jax.experimental.pallas import tpu as pltpu
from jax.sharding import Mesh
from jax.sharding import PartitionSpec as P


DP = ("zl", "y", "x")
TP = ("zh", "c")
F32 = jnp.float32
BF16 = jnp.bfloat16


def exchange(blocks, axes):
    return lax.all_to_all(blocks, axes, 0, 0, tiled=True)


def total(blocks):
    return jnp.sum(blocks.astype(F32), axis=0)


def shifted(block, axis, shift):
    peers = lax.axis_size(axis)
    return lax.ppermute(block, axis, [(i, (i + shift) % peers) for i in range(peers)])


def swapped(block, axis, bit):
    return lax.ppermute(block, axis, [(i, i ^ bit) for i in range(lax.axis_size(axis))])


def owner_columns(cols, x_index):
    zl, y, x = (lax.axis_size(a) for a in DP)
    rows = cols // (zl * y * x)
    place = jnp.arange(cols)
    shift, owner, row = place // (zl * y * rows), place // rows % (zl * y), place % rows
    source = owner * (x * rows) + lax.rem(shift + x_index, x) * rows + row
    return (place[:, None] == source[None, :]).astype(BF16)


def pack_kernel(first, second, third, fourth, rider, packed):
    owners, rows, _ = packed.shape
    width = first.shape[1]
    per_tile = 8 // rows
    for tile in range(owners // per_tile):
        place = slice(tile * 8, tile * 8 + 8)
        parts = [ref[place, :].astype(F32) for ref in (first, second, third, fourth)]
        summed = (parts[0] + parts[1]) + (parts[2] + parts[3])
        for one in range(per_tile):
            owner = tile * per_tile + one
            packed[owner, :, :width] = summed[one * rows : (one + 1) * rows, :].astype(BF16)
            packed[owner, :, width:] = rider[...]


def pack(blocks, rider):
    share, width = blocks[0].shape
    rows, extra = rider.shape
    shape = (share // rows, rows, width + extra)
    return pl.pallas_call(
        pack_kernel,
        out_shape=jax.ShapeDtypeStruct(shape, BF16),
        in_specs=[pl.BlockSpec(memory_space=pltpu.VMEM)] * 5,
        out_specs=pl.BlockSpec(memory_space=pltpu.VMEM),
        compiler_params=pltpu.CompilerParams(vmem_limit_bytes=10 * 2**20),
        cost_estimate=pl.CostEstimate(
            flops=3 * share * width, bytes_accessed=10 * share * width, transcendentals=0
        ),
        name="pack",
    )(*blocks, rider)


def rows_kernel(summands, resid, gain, grad_in, rows):
    summed = [summands[i].astype(F32) for i in range(summands.shape[0])]
    dnormed = (summed[0] + summed[1]) + (summed[2] + summed[3])
    resid_f = resid[...].astype(F32)
    inv = lax.rsqrt(jnp.mean(resid_f * resid_f, axis=-1, keepdims=True) + 1e-05)
    unit = resid_f * inv
    dunit = dnormed * gain[...].astype(F32)
    inner = jnp.mean(dunit * unit, axis=-1, keepdims=True)
    rows[...] = (grad_in[...].astype(F32) + inv * (dunit - unit * inner)).astype(BF16)


def result_rows(summands, resid, gain, grad_in):
    rows, width = resid.shape
    return pl.pallas_call(
        rows_kernel,
        out_shape=jax.ShapeDtypeStruct((rows, width), BF16),
        in_specs=[pl.BlockSpec(memory_space=pltpu.VMEM)] * 4,
        out_specs=pl.BlockSpec(memory_space=pltpu.VMEM),
        compiler_params=pltpu.CompilerParams(vmem_limit_bytes=10 * 2**20),
        cost_estimate=pl.CostEstimate(
            flops=15 * rows * width, bytes_accessed=14 * rows * width, transcendentals=0
        ),
        name="result_rows",
    )(summands, resid, gain, grad_in)


def body(resid, gain, grad_q, w_query, grad_in):
    tokens, width = resid.shape
    cols = grad_q.shape[1]
    core, zh = lax.axis_index("c"), lax.axis_index("zh")
    n_zh, n_x, n_y, n_zl = (lax.axis_size(a) for a in ("zh", "x", "y", "zl"))
    half = tokens // 2
    own = half // n_zh
    gain_f = gain.astype(F32)

    def rows_of(array, start, size):
        return lax.dynamic_slice_in_dim(array, start, size, 0)

    def inverse(rows):
        rows_f = rows.astype(F32)
        return lax.rsqrt(jnp.mean(rows_f * rows_f, axis=-1, keepdims=True) + 1e-05)

    def term(start):
        rows = rows_of(grad_q, start, half)
        return jnp.dot(rows, w_query, preferred_element_type=F32).astype(BF16)

    inv, grad_q = lax.optimization_barrier((inverse(resid), grad_q))
    ordered = jnp.dot(grad_q, owner_columns(cols, lax.axis_index("x")), preferred_element_type=F32)
    ordered = ordered.astype(BF16)

    other_start, own_start = (1 - core) * half, core * half
    sent = term(other_start)
    got = swapped(sent, "c", 1)
    kept = lax.optimization_barrier(term(own_start))
    pair = (kept.astype(F32) + got.astype(F32)).astype(BF16)
    pair, inv, ordered = lax.optimization_barrier((pair, inv, ordered))
    summands = exchange(pair.reshape(n_zh, own, width), "zh")

    unit = resid.astype(F32) * inv
    part = jnp.sum(sent.astype(F32) * rows_of(unit, other_start, half), axis=0)
    part = part + jnp.sum(kept.astype(F32) * rows_of(unit, own_start, half), axis=0)
    part, inv_x = lax.optimization_barrier((part.reshape(n_y, -1, 128), inv))
    part = part + swapped(part, "y", 1)

    normed = (resid.astype(F32) * inv_x * gain_f).astype(BF16)
    share = cols // n_x

    def block(shift):
        columns = ordered[:, shift * share : (shift + 1) * share]
        local = lax.dot_general(
            columns, normed, (((0,), (0,)), ((), ())), preferred_element_type=F32
        )
        return lax.optimization_barrier(local.astype(BF16))

    blocks = [block(s) for s in range(n_x)]
    blocks = [b if s == 0 else shifted(b, "x", s) for s, b in enumerate(blocks)]
    part = part + swapped(part, "y", 2)
    first = own_start + zh * own
    ready = (blocks[0], rows_of(resid, first, own), rows_of(grad_in, first, own))
    part, own_block, resid_rows, grad_rows = lax.optimization_barrier((part, *ready))
    part = part + swapped(part, "y", 4)
    part = lax.dynamic_index_in_dim(part, lax.axis_index("y"), 0, keepdims=False)

    axes = ("x", "zh", "c")
    part, summands = lax.optimization_barrier((part, summands))
    part = jnp.broadcast_to(part[None], (lax.axis_size(axes), *part.shape))
    part = total(exchange(part, axes))
    rows = result_rows(summands, resid_rows, gain.reshape(1, width), grad_rows)

    upper = part.astype(BF16)
    lower = (part - upper.astype(F32)).astype(BF16)
    packed = pack([own_block, *blocks[1:]], jnp.concatenate([upper, lower], axis=1))
    last = exchange(packed, ("zl", "y"))
    weight_grad = total(last[:, :, :width])
    parts = last[:, :, width:].astype(F32)
    parts = (parts[:, :, :128] + parts[:, :, 128:]).reshape(n_zl, n_y, -1, 128)
    gain_grad = jnp.sum(parts, axis=0).reshape(-1)

    result = jnp.zeros((tokens, width), BF16)
    for shift in (0, 1, n_zh - 1, 2):
        piece = rows if shift == 0 else shifted(rows, "zh", shift)
        other = swapped(piece, "c", 1)
        source = lax.rem(zh + n_zh - shift, n_zh) * own
        result = lax.dynamic_update_slice_in_dim(result, piece, own_start + source, 0)
        result = lax.dynamic_update_slice_in_dim(result, other, other_start + source, 0)
    return weight_grad, gain_grad, result


def solution(mesh):
    finer = Mesh(mesh.devices.reshape(3, 8, 4, 4, 2), ("zl", "y", "x", "zh", "c"))
    in_specs = (P(DP, None), P(), P(DP, TP), P(TP, None), P(DP, None))
    out_specs = (P(TP + DP, None), P(), P(DP, None))
    return jax.shard_map(body, mesh=finer, in_specs=in_specs, out_specs=out_specs, check_vma=False)
```

```python
import jax
import jax.numpy as jnp
from jax import lax
from jax.experimental import pallas as pl
from jax.experimental.pallas import tpu as pltpu
from jax.sharding import Mesh
from jax.sharding import PartitionSpec as P


DP = ("zl", "y", "x")
TP = ("zh", "c")
F32 = jnp.float32
BF16 = jnp.bfloat16


def exchange(blocks, axes):
    return lax.all_to_all(blocks, axes, 0, 0, tiled=True)


def total(blocks):
    return jnp.sum(blocks.astype(F32), axis=0)


def shifted(block, axis, shift):
    peers = lax.axis_size(axis)
    return lax.ppermute(block, axis, [(i, (i + shift) % peers) for i in range(peers)])


def swapped(block, axis, bit):
    return lax.ppermute(block, axis, [(i, i ^ bit) for i in range(lax.axis_size(axis))])


def owner_columns(cols, x_index):
    zl, y, x = (lax.axis_size(a) for a in DP)
    rows = cols // (zl * y * x)
    place = jnp.arange(cols)
    shift, owner, row = place // (zl * y * rows), place // rows % (zl * y), place % rows
    source = owner * (x * rows) + lax.rem(shift + x_index, x) * rows + row
    return (place[:, None] == source[None, :]).astype(BF16)


def pack_kernel(first, second, third, fourth, rider, packed):
    owners, rows, _ = packed.shape
    width = first.shape[1]
    per_tile = 8 // rows
    for tile in range(owners // per_tile):
        place = slice(tile * 8, tile * 8 + 8)
        parts = [ref[place, :].astype(F32) for ref in (first, second, third, fourth)]
        summed = (parts[0] + parts[1]) + (parts[2] + parts[3])
        for one in range(per_tile):
            owner = tile * per_tile + one
            packed[owner, :, :width] = summed[one * rows : (one + 1) * rows, :].astype(BF16)
            packed[owner, :, width:] = rider[...]


def pack(blocks, rider):
    share, width = blocks[0].shape
    rows, extra = rider.shape
    shape = (share // rows, rows, width + extra)
    return pl.pallas_call(
        pack_kernel,
        out_shape=jax.ShapeDtypeStruct(shape, BF16),
        in_specs=[pl.BlockSpec(memory_space=pltpu.VMEM)] * 5,
        out_specs=pl.BlockSpec(memory_space=pltpu.VMEM),
        compiler_params=pltpu.CompilerParams(vmem_limit_bytes=10 * 2**20),
        cost_estimate=pl.CostEstimate(
            flops=3 * share * width, bytes_accessed=10 * share * width, transcendentals=0
        ),
        name="pack",
    )(*blocks, rider)


def sums_kernel(last, weight_grad, gain_grad):
    width = weight_grad.shape[1]
    summed = last[0].astype(F32)
    for one in range(1, last.shape[0]):
        summed = summed + last[one].astype(F32)
    weight_grad[...] = summed[:, :width]
    extra = summed.shape[1] - width
    for row in range(summed.shape[0]):
        gain_grad[:, row * extra : (row + 1) * extra] = summed[row : row + 1, width:]


def last_sums(last, width):
    peers, rows, lanes = last.shape
    return pl.pallas_call(
        sums_kernel,
        out_shape=(
            jax.ShapeDtypeStruct((rows, width), F32),
            jax.ShapeDtypeStruct((1, rows * (lanes - width)), F32),
        ),
        in_specs=[pl.BlockSpec(memory_space=pltpu.VMEM)],
        out_specs=[pl.BlockSpec(memory_space=pltpu.VMEM)] * 2,
        compiler_params=pltpu.CompilerParams(vmem_limit_bytes=10 * 2**20),
        cost_estimate=pl.CostEstimate(
            flops=peers * rows * lanes, bytes_accessed=2 * peers * rows * lanes, transcendentals=0
        ),
        name="last_sums",
    )(last)


def rows_kernel(first, summands, gain, resid, grad_in, rows, held, sems):
    place = pl.ds(pl.multiple_of(first[0], 32), rows.shape[0])
    copies = [
        pltpu.make_async_copy(array.at[place, :], held.at[i], sems.at[i])
        for i, array in enumerate((resid, grad_in))
    ]
    for copy in copies:
        copy.start()
    summed = [summands[i].astype(F32) for i in range(summands.shape[0])]
    dunit = ((summed[0] + summed[1]) + (summed[2] + summed[3])) * gain[...].astype(F32)
    copies[0].wait()
    resid_f = held[0].astype(F32)
    inv = lax.rsqrt(jnp.mean(resid_f * resid_f, axis=-1, keepdims=True) + 1e-05)
    unit = resid_f * inv
    inner = jnp.mean(dunit * unit, axis=-1, keepdims=True)
    copies[1].wait()
    rows[...] = (held[1].astype(F32) + inv * (dunit - unit * inner)).astype(BF16)


def result_rows(first, summands, gain, resid, grad_in):
    _, rows, width = summands.shape
    return pl.pallas_call(
        rows_kernel,
        out_shape=jax.ShapeDtypeStruct((rows, width), BF16),
        in_specs=[
            pl.BlockSpec(memory_space=pltpu.SMEM),
            pl.BlockSpec(memory_space=pltpu.VMEM),
            pl.BlockSpec(memory_space=pltpu.VMEM),
            pl.BlockSpec(memory_space=pltpu.HBM),
            pl.BlockSpec(memory_space=pltpu.HBM),
        ],
        out_specs=pl.BlockSpec(memory_space=pltpu.VMEM),
        scratch_shapes=[pltpu.VMEM((2, rows, width), BF16), pltpu.SemaphoreType.DMA((2,))],
        compiler_params=pltpu.CompilerParams(vmem_limit_bytes=125 * 2**19),
        cost_estimate=pl.CostEstimate(
            flops=15 * rows * width, bytes_accessed=14 * rows * width, transcendentals=0
        ),
        name="result_rows",
    )(first, summands, gain, resid, grad_in)


def body(resid, gain, grad_q, w_query, grad_in):
    tokens, width = resid.shape
    cols = grad_q.shape[1]
    core, zh = lax.axis_index("c"), lax.axis_index("zh")
    n_zh, n_x, n_y, n_zl = (lax.axis_size(a) for a in ("zh", "x", "y", "zl"))
    half = tokens // 2
    own = half // n_zh
    gain_f = gain.astype(F32)

    def rows_of(array, start, size):
        return lax.dynamic_slice_in_dim(array, start, size, 0)

    def inverse(rows):
        rows_f = rows.astype(F32)
        return lax.rsqrt(jnp.mean(rows_f * rows_f, axis=-1, keepdims=True) + 1e-05)

    def term(start):
        rows = rows_of(grad_q, start, half)
        return jnp.dot(rows, w_query, preferred_element_type=F32).astype(BF16)

    inv, grad_q = lax.optimization_barrier((inverse(resid), grad_q))
    ordered = jnp.dot(grad_q, owner_columns(cols, lax.axis_index("x")), preferred_element_type=F32)
    ordered = ordered.astype(BF16)

    other_start, own_start = (1 - core) * half, core * half
    sent = term(other_start)
    got = swapped(sent, "c", 1)
    kept = lax.optimization_barrier(term(own_start))
    pair = (kept.astype(F32) + got.astype(F32)).astype(BF16)
    pair, inv, ordered = lax.optimization_barrier((pair, inv, ordered))
    summands = exchange(pair.reshape(n_zh, own, width), "zh")

    unit = resid.astype(F32) * inv
    part = jnp.sum(sent.astype(F32) * rows_of(unit, other_start, half), axis=0)
    part = part + jnp.sum(kept.astype(F32) * rows_of(unit, own_start, half), axis=0)
    part, inv_x = lax.optimization_barrier((part.reshape(-1, 128), inv))
    part = part + swapped(part, "x", 1)
    part, inv_x = lax.optimization_barrier((part, inv_x))
    part_x = swapped(part, "x", 2)

    normed = (resid.astype(F32) * inv_x * gain_f).astype(BF16)
    share = cols // n_x

    def block(shift):
        columns = ordered[:, shift * share : (shift + 1) * share]
        local = lax.dot_general(
            columns, normed, (((0,), (0,)), ((), ())), preferred_element_type=F32
        )
        return lax.optimization_barrier(local.astype(BF16))

    blocks = [block(s) for s in range(n_x)]
    blocks = [b if s == 0 else shifted(b, "x", s) for s, b in enumerate(blocks)]
    first = (own_start + zh * own).astype(jnp.int32).reshape(1)
    ready = (part + part_x, blocks[0], first, gain.reshape(1, width))
    part, own_block, first, gain_row = lax.optimization_barrier(ready)

    part, summands = lax.optimization_barrier((part, summands))
    part = jnp.broadcast_to(part[None], (lax.axis_size(TP), *part.shape))
    part = total(exchange(part, TP))
    rows = result_rows(first, summands, gain_row, resid, grad_in)

    mine = share // (n_y * n_zl)
    packed = pack([own_block, *blocks[1:]], part.astype(BF16).reshape(mine, -1))
    last = exchange(packed, ("zl", "y"))
    weight_grad, gain_grad = last_sums(last, width)

    result = jnp.zeros((tokens, width), BF16)
    for shift in (0, 1, n_zh - 1, 2):
        piece = rows if shift == 0 else shifted(rows, "zh", shift)
        other = swapped(piece, "c", 1)
        source = lax.rem(zh + n_zh - shift, n_zh) * own
        result = lax.dynamic_update_slice_in_dim(result, piece, own_start + source, 0)
        result = lax.dynamic_update_slice_in_dim(result, other, other_start + source, 0)
    return weight_grad, gain_grad.reshape(-1), result


def solution(mesh):
    finer = Mesh(mesh.devices.reshape(3, 8, 4, 4, 2), ("zl", "y", "x", "zh", "c"))
    in_specs = (P(DP, None), P(), P(DP, TP), P(TP, None), P(DP, None))
    out_specs = (P(TP + DP, None), P(), P(DP, None))
    return jax.shard_map(body, mesh=finer, in_specs=in_specs, out_specs=out_specs, check_vma=False)
```

```python
import jax
import jax.numpy as jnp
from jax import lax
from jax.experimental import pallas as pl
from jax.experimental.pallas import tpu as pltpu
from jax.sharding import Mesh
from jax.sharding import PartitionSpec as P


DP = ("zl", "y", "x")
TP = ("zh", "c")
F32 = jnp.float32
BF16 = jnp.bfloat16


def exchange(blocks, axes):
    return lax.all_to_all(blocks, axes, 0, 0, tiled=True)


def total(blocks):
    return jnp.sum(blocks.astype(F32), axis=0)


def shifted(block, axis, shift):
    peers = lax.axis_size(axis)
    return lax.ppermute(block, axis, [(i, (i + shift) % peers) for i in range(peers)])


def swapped(block, axis, bit):
    return lax.ppermute(block, axis, [(i, i ^ bit) for i in range(lax.axis_size(axis))])


def owner_columns(cols, x_index):
    zl, y, x = (lax.axis_size(a) for a in DP)
    rows = cols // (zl * y * x)
    place = jnp.arange(cols)
    shift, owner, row = place // (zl * y * rows), place // rows % (zl * y), place % rows
    source = owner * (x * rows) + lax.rem(shift + x_index, x) * rows + row
    return (place[:, None] == source[None, :]).astype(BF16)


def pack_kernel(first, second, third, fourth, rider, packed):
    owners, rows, _ = packed.shape
    width = first.shape[1]
    per_tile = 8 // rows
    for tile in range(owners // per_tile):
        place = slice(tile * 8, tile * 8 + 8)
        parts = [ref[place, :].astype(F32) for ref in (first, second, third, fourth)]
        summed = (parts[0] + parts[1]) + (parts[2] + parts[3])
        for one in range(per_tile):
            owner = tile * per_tile + one
            packed[owner, :, :width] = summed[one * rows : (one + 1) * rows, :].astype(BF16)
            packed[owner, :, width:] = rider[...]


def pack(blocks, rider):
    share, width = blocks[0].shape
    rows, extra = rider.shape
    shape = (share // rows, rows, width + extra)
    return pl.pallas_call(
        pack_kernel,
        out_shape=jax.ShapeDtypeStruct(shape, BF16),
        in_specs=[pl.BlockSpec(memory_space=pltpu.VMEM)] * 5,
        out_specs=pl.BlockSpec(memory_space=pltpu.VMEM),
        compiler_params=pltpu.CompilerParams(vmem_limit_bytes=10 * 2**20),
        cost_estimate=pl.CostEstimate(
            flops=3 * share * width, bytes_accessed=10 * share * width, transcendentals=0
        ),
        name="pack",
    )(*blocks, rider)


def sums_kernel(last, weight_grad, gain_grad):
    width = weight_grad.shape[1]
    summed = last[0].astype(F32)
    for one in range(1, last.shape[0]):
        summed = summed + last[one].astype(F32)
    weight_grad[...] = summed[:, :width]
    extra = summed.shape[1] - width
    for row in range(summed.shape[0]):
        gain_grad[:, row * extra : (row + 1) * extra] = summed[row : row + 1, width:]


def last_sums(last, width):
    peers, rows, lanes = last.shape
    return pl.pallas_call(
        sums_kernel,
        out_shape=(
            jax.ShapeDtypeStruct((rows, width), F32),
            jax.ShapeDtypeStruct((1, rows * (lanes - width)), F32),
        ),
        in_specs=[pl.BlockSpec(memory_space=pltpu.VMEM)],
        out_specs=[pl.BlockSpec(memory_space=pltpu.VMEM)] * 2,
        compiler_params=pltpu.CompilerParams(vmem_limit_bytes=10 * 2**20),
        cost_estimate=pl.CostEstimate(
            flops=peers * rows * lanes, bytes_accessed=2 * peers * rows * lanes, transcendentals=0
        ),
        name="last_sums",
    )(last)


def rows_kernel(summands, gain, slices, rows):
    summed = [summands[i].astype(F32) for i in range(summands.shape[0])]
    dunit = ((summed[0] + summed[1]) + (summed[2] + summed[3])) * gain[...].astype(F32)
    resid_f = slices[0].astype(F32)
    inv = lax.rsqrt(jnp.mean(resid_f * resid_f, axis=-1, keepdims=True) + 1e-05)
    unit = resid_f * inv
    inner = jnp.mean(dunit * unit, axis=-1, keepdims=True)
    rows[...] = (slices[1].astype(F32) + inv * (dunit - unit * inner)).astype(BF16)


def result_rows(summands, gain, slices):
    _, rows, width = slices.shape
    return pl.pallas_call(
        rows_kernel,
        out_shape=jax.ShapeDtypeStruct((rows, width), BF16),
        in_specs=[pl.BlockSpec(memory_space=pltpu.VMEM)] * 3,
        out_specs=pl.BlockSpec(memory_space=pltpu.VMEM),
        compiler_params=pltpu.CompilerParams(vmem_limit_bytes=10 * 2**20),
        cost_estimate=pl.CostEstimate(
            flops=15 * rows * width, bytes_accessed=14 * rows * width, transcendentals=0
        ),
        name="result_rows",
    )(summands, gain, slices)


def body(resid, gain, grad_q, w_query, grad_in):
    tokens, width = resid.shape
    cols = grad_q.shape[1]
    core, zh = lax.axis_index("c"), lax.axis_index("zh")
    n_zh, n_x, n_y, n_zl = (lax.axis_size(a) for a in ("zh", "x", "y", "zl"))
    half = tokens // 2
    own = half // n_zh
    gain_f = gain.astype(F32)

    def rows_of(array, start, size):
        return lax.dynamic_slice_in_dim(array, start, size, 0)

    def inverse(rows):
        rows_f = rows.astype(F32)
        return lax.rsqrt(jnp.mean(rows_f * rows_f, axis=-1, keepdims=True) + 1e-05)

    def term(start):
        rows = rows_of(grad_q, start, half)
        return jnp.dot(rows, w_query, preferred_element_type=F32).astype(BF16)

    inv, grad_q = lax.optimization_barrier((inverse(resid), grad_q))

    other_start, own_start = (1 - core) * half, core * half
    sent = term(other_start)
    got = swapped(sent, "c", 1)
    kept = lax.optimization_barrier(term(own_start))
    pair = (kept.astype(F32) + got.astype(F32)).astype(BF16)
    held = (pair, inv, grad_q, resid, grad_in)
    pair, inv, grad_q, resid_x, grad_in = lax.optimization_barrier(held)
    summands = exchange(pair.reshape(n_zh, own, width), "zh")

    unit = resid.astype(F32) * inv
    part = jnp.sum(sent.astype(F32) * rows_of(unit, other_start, half), axis=0)
    part = part + jnp.sum(kept.astype(F32) * rows_of(unit, own_start, half), axis=0)
    part, inv_x = lax.optimization_barrier((part.reshape(-1, 128), inv))
    ordered = jnp.dot(grad_q, owner_columns(cols, lax.axis_index("x")), preferred_element_type=F32)
    ordered = lax.optimization_barrier(ordered.astype(BF16))
    part = part + swapped(part, "x", 1)
    part, inv_x = lax.optimization_barrier((part, inv_x))
    part_x = swapped(part, "x", 2)

    normed = (resid.astype(F32) * inv_x * gain_f).astype(BF16)
    share = cols // n_x

    def block(shift):
        columns = ordered[:, shift * share : (shift + 1) * share]
        local = lax.dot_general(
            columns, normed, (((0,), (0,)), ((), ())), preferred_element_type=F32
        )
        return lax.optimization_barrier(local.astype(BF16))

    blocks = [block(s) for s in range(n_x)]
    blocks = [b if s == 0 else shifted(b, "x", s) for s, b in enumerate(blocks)]
    first = own_start + zh * own
    slices = jnp.stack([rows_of(resid_x, first, own), rows_of(grad_in, first, own)])
    ready = (part + part_x, blocks[0], gain.reshape(1, width), slices)
    part, own_block, gain_row, slices = lax.optimization_barrier(ready)

    part, summands = lax.optimization_barrier((part, summands))
    part = jnp.broadcast_to(part[None], (lax.axis_size(TP), *part.shape))
    part = total(exchange(part, TP))
    rows = result_rows(summands, gain_row, slices)

    mine = share // (n_y * n_zl)
    packed = pack([own_block, *blocks[1:]], part.astype(BF16).reshape(mine, -1))
    last = exchange(packed, ("zl", "y"))
    weight_grad, gain_grad = last_sums(last, width)

    before, after = shifted(rows, "zh", 1), shifted(rows, "zh", n_zh - 1)
    upper, lower = before[: own // 2], after[own // 2 :]
    upper, lower = shifted(upper, "zh", 1), shifted(lower, "zh", n_zh - 1)
    pieces = (
        (0, 0, rows), (1, 0, before), (n_zh - 1, 0, after), (2, 0, upper), (2, own // 2, lower)
    )
    result = jnp.zeros((tokens, width), BF16)
    for shift, offset, piece in pieces:
        other = swapped(piece, "c", 1)
        source = lax.rem(zh + n_zh - shift, n_zh) * own + offset
        result = lax.dynamic_update_slice_in_dim(result, piece, own_start + source, 0)
        result = lax.dynamic_update_slice_in_dim(result, other, other_start + source, 0)
    return weight_grad, gain_grad.reshape(-1), result


def solution(mesh):
    finer = Mesh(mesh.devices.reshape(3, 8, 4, 4, 2), ("zl", "y", "x", "zh", "c"))
    in_specs = (P(DP, None), P(), P(DP, TP), P(TP, None), P(DP, None))
    out_specs = (P(TP + DP, None), P(), P(DP, None))
    return jax.shard_map(body, mesh=finer, in_specs=in_specs, out_specs=out_specs, check_vma=False)
```

```python
import jax
import jax.numpy as jnp
from jax import lax
from jax.experimental import pallas as pl
from jax.experimental.pallas import tpu as pltpu
from jax.sharding import Mesh
from jax.sharding import PartitionSpec as P


DP = ("zl", "y", "x")
TP = ("zh", "c")
F32 = jnp.float32
BF16 = jnp.bfloat16


def exchange(blocks, axes):
    return lax.all_to_all(blocks, axes, 0, 0, tiled=True)


def total(blocks):
    return jnp.sum(blocks.astype(F32), axis=0)


def shifted(block, axis, shift):
    peers = lax.axis_size(axis)
    return lax.ppermute(block, axis, [(i, (i + shift) % peers) for i in range(peers)])


def swapped(block, axis, bit):
    return lax.ppermute(block, axis, [(i, i ^ bit) for i in range(lax.axis_size(axis))])


def owner_columns(cols, x_index):
    zl, y, x = (lax.axis_size(a) for a in DP)
    rows = cols // (zl * y * x)
    place = jnp.arange(cols)
    shift, owner, row = place // (zl * y * rows), place // rows % (zl * y), place % rows
    source = owner * (x * rows) + lax.rem(shift + x_index, x) * rows + row
    return (place[:, None] == source[None, :]).astype(BF16)


def pack_kernel(first, second, third, fourth, rider, packed):
    owners, rows, _ = packed.shape
    width = first.shape[1]
    per_tile = 8 // rows
    for tile in range(owners // per_tile):
        place = slice(tile * 8, tile * 8 + 8)
        parts = [ref[place, :].astype(F32) for ref in (first, second, third, fourth)]
        summed = (parts[0] + parts[1]) + (parts[2] + parts[3])
        for one in range(per_tile):
            owner = tile * per_tile + one
            packed[owner, :, :width] = summed[one * rows : (one + 1) * rows, :].astype(BF16)
            packed[owner, :, width:] = rider[...]


def pack(blocks, rider):
    share, width = blocks[0].shape
    rows, extra = rider.shape
    shape = (share // rows, rows, width + extra)
    return pl.pallas_call(
        pack_kernel,
        out_shape=jax.ShapeDtypeStruct(shape, BF16),
        in_specs=[pl.BlockSpec(memory_space=pltpu.VMEM)] * 5,
        out_specs=pl.BlockSpec(memory_space=pltpu.VMEM),
        compiler_params=pltpu.CompilerParams(vmem_limit_bytes=10 * 2**20),
        cost_estimate=pl.CostEstimate(
            flops=3 * share * width, bytes_accessed=10 * share * width, transcendentals=0
        ),
        name="pack",
    )(*blocks, rider)


def sums_kernel(last, weight_grad, gain_grad):
    width = weight_grad.shape[1]
    summed = last[0].astype(F32)
    for one in range(1, last.shape[0]):
        summed = summed + last[one].astype(F32)
    weight_grad[...] = summed[:, :width]
    extra = summed.shape[1] - width
    for row in range(summed.shape[0]):
        gain_grad[:, row * extra : (row + 1) * extra] = summed[row : row + 1, width:]


def last_sums(last, width):
    peers, rows, lanes = last.shape
    return pl.pallas_call(
        sums_kernel,
        out_shape=(
            jax.ShapeDtypeStruct((rows, width), F32),
            jax.ShapeDtypeStruct((1, rows * (lanes - width)), F32),
        ),
        in_specs=[pl.BlockSpec(memory_space=pltpu.VMEM)],
        out_specs=[pl.BlockSpec(memory_space=pltpu.VMEM)] * 2,
        compiler_params=pltpu.CompilerParams(vmem_limit_bytes=10 * 2**20),
        cost_estimate=pl.CostEstimate(
            flops=peers * rows * lanes, bytes_accessed=2 * peers * rows * lanes, transcendentals=0
        ),
        name="last_sums",
    )(last)


def rows_kernel(summands, gain, slices, rows):
    summed = [summands[i].astype(F32) for i in range(summands.shape[0])]
    dunit = ((summed[0] + summed[1]) + (summed[2] + summed[3])) * gain[...].astype(F32)
    resid_f = slices[0].astype(F32)
    inv = lax.rsqrt(jnp.mean(resid_f * resid_f, axis=-1, keepdims=True) + 1e-05)
    unit = resid_f * inv
    inner = jnp.mean(dunit * unit, axis=-1, keepdims=True)
    rows[...] = (slices[1].astype(F32) + inv * (dunit - unit * inner)).astype(BF16)


def result_rows(summands, gain, slices):
    _, rows, width = slices.shape
    return pl.pallas_call(
        rows_kernel,
        out_shape=jax.ShapeDtypeStruct((rows, width), BF16),
        in_specs=[pl.BlockSpec(memory_space=pltpu.VMEM)] * 3,
        out_specs=pl.BlockSpec(memory_space=pltpu.VMEM),
        compiler_params=pltpu.CompilerParams(vmem_limit_bytes=10 * 2**20),
        cost_estimate=pl.CostEstimate(
            flops=15 * rows * width, bytes_accessed=14 * rows * width, transcendentals=0
        ),
        name="result_rows",
    )(summands, gain, slices)


def body(resid, gain, grad_q, w_query, grad_in):
    tokens, width = resid.shape
    cols = grad_q.shape[1]
    core, zh = lax.axis_index("c"), lax.axis_index("zh")
    n_zh, n_x, n_y, n_zl = (lax.axis_size(a) for a in ("zh", "x", "y", "zl"))
    half = tokens // 2
    own = half // n_zh
    gain_f = gain.astype(F32)

    def rows_of(array, start, size):
        return lax.dynamic_slice_in_dim(array, start, size, 0)

    def inverse(rows):
        rows_f = rows.astype(F32)
        return lax.rsqrt(jnp.mean(rows_f * rows_f, axis=-1, keepdims=True) + 1e-05)

    def term(start):
        rows = rows_of(grad_q, start, half)
        return jnp.dot(rows, w_query, preferred_element_type=F32).astype(BF16)

    inv, grad_q = lax.optimization_barrier((inverse(resid), grad_q))

    other_start, own_start = (1 - core) * half, core * half
    sent = term(other_start)
    got = swapped(sent, "c", 1)
    kept = lax.optimization_barrier(term(own_start))
    pair = (kept.astype(F32) + got.astype(F32)).astype(BF16)
    held = (pair, inv, grad_q, resid, grad_in)
    pair, inv, grad_q, resid_x, grad_in = lax.optimization_barrier(held)
    summands = exchange(pair.reshape(n_zh, own, width), "zh")

    unit = resid.astype(F32) * inv
    part = jnp.sum(sent.astype(F32) * rows_of(unit, other_start, half), axis=0)
    part = part + jnp.sum(kept.astype(F32) * rows_of(unit, own_start, half), axis=0)
    part, inv_x = lax.optimization_barrier((part.reshape(-1, 128), inv))
    ordered = jnp.dot(grad_q, owner_columns(cols, lax.axis_index("x")), preferred_element_type=F32)
    ordered = lax.optimization_barrier(ordered.astype(BF16))
    part = part + swapped(part, "x", 1)
    part, inv_x = lax.optimization_barrier((part, inv_x))
    part_x = swapped(part, "x", 2)

    normed = (resid.astype(F32) * inv_x * gain_f).astype(BF16)
    share = cols // n_x

    def block(shift):
        columns = ordered[:, shift * share : (shift + 1) * share]
        local = lax.dot_general(
            columns, normed, (((0,), (0,)), ((), ())), preferred_element_type=F32
        )
        return lax.optimization_barrier(local.astype(BF16))

    blocks = [block(s) for s in range(n_x)]
    blocks = [b if s == 0 else shifted(b, "x", s) for s, b in enumerate(blocks)]
    first = own_start + zh * own
    slices = jnp.stack([rows_of(resid_x, first, own), rows_of(grad_in, first, own)])
    ready = (part + part_x, blocks[0], gain.reshape(1, width), slices)
    part, own_block, gain_row, slices = lax.optimization_barrier(ready)

    part, summands = lax.optimization_barrier((part, summands))
    part = jnp.broadcast_to(part[None], (lax.axis_size(TP), *part.shape))
    part = total(exchange(part, TP))
    rows = result_rows(summands, gain_row, slices)

    mine = share // (n_y * n_zl)
    packed = pack([own_block, *blocks[1:]], part.astype(BF16).reshape(mine, -1))
    last = exchange(packed, ("zl", "y"))
    weight_grad, gain_grad = last_sums(last, width)

    result = jnp.zeros((tokens, width), BF16)
    for shift in (0, 1, n_zh - 1, 2):
        piece = rows if shift == 0 else shifted(rows, "zh", shift)
        other = swapped(piece, "c", 1)
        source = lax.rem(zh + n_zh - shift, n_zh) * own
        result = lax.dynamic_update_slice_in_dim(result, piece, own_start + source, 0)
        result = lax.dynamic_update_slice_in_dim(result, other, other_start + source, 0)
    return weight_grad, gain_grad.reshape(-1), result


def solution(mesh):
    finer = Mesh(mesh.devices.reshape(3, 8, 4, 4, 2), ("zl", "y", "x", "zh", "c"))
    in_specs = (P(DP, None), P(), P(DP, TP), P(TP, None), P(DP, None))
    out_specs = (P(TP + DP, None), P(), P(DP, None))
    return jax.shard_map(body, mesh=finer, in_specs=in_specs, out_specs=out_specs, check_vma=False)
```

```python
import jax
import jax.numpy as jnp
from jax import lax
from jax.experimental import pallas as pl
from jax.experimental.pallas import tpu as pltpu
from jax.sharding import Mesh
from jax.sharding import PartitionSpec as P


DP = ("zl", "y", "x")
TP = ("zh", "c")
F32 = jnp.float32
BF16 = jnp.bfloat16


def exchange(blocks, axes):
    return lax.all_to_all(blocks, axes, 0, 0, tiled=True)


def total(blocks):
    return jnp.sum(blocks.astype(F32), axis=0)


def shifted(block, axis, shift):
    peers = lax.axis_size(axis)
    return lax.ppermute(block, axis, [(i, (i + shift) % peers) for i in range(peers)])


def swapped(block, axis, bit):
    return lax.ppermute(block, axis, [(i, i ^ bit) for i in range(lax.axis_size(axis))])


def owner_columns(cols, x_index):
    zl, y, x = (lax.axis_size(a) for a in DP)
    rows = cols // (zl * y * x)
    place = jnp.arange(cols)
    shift, owner, row = place // (zl * y * rows), place // rows % (zl * y), place % rows
    source = owner * (x * rows) + lax.rem(shift + x_index, x) * rows + row
    return (place[:, None] == source[None, :]).astype(BF16)


def pack_kernel(first, second, third, fourth, rider, packed):
    owners, rows, _ = packed.shape
    width = first.shape[1]
    per_tile = 8 // rows
    for tile in range(owners // per_tile):
        place = slice(tile * 8, tile * 8 + 8)
        parts = [ref[place, :].astype(F32) for ref in (first, second, third, fourth)]
        summed = (parts[0] + parts[1]) + (parts[2] + parts[3])
        for one in range(per_tile):
            owner = tile * per_tile + one
            packed[owner, :, :width] = summed[one * rows : (one + 1) * rows, :].astype(BF16)
            packed[owner, :, width:] = rider[...]


def pack(blocks, rider):
    share, width = blocks[0].shape
    rows, extra = rider.shape
    shape = (share // rows, rows, width + extra)
    return pl.pallas_call(
        pack_kernel,
        out_shape=jax.ShapeDtypeStruct(shape, BF16),
        in_specs=[pl.BlockSpec(memory_space=pltpu.VMEM)] * 5,
        out_specs=pl.BlockSpec(memory_space=pltpu.VMEM),
        compiler_params=pltpu.CompilerParams(vmem_limit_bytes=10 * 2**20),
        cost_estimate=pl.CostEstimate(
            flops=3 * share * width, bytes_accessed=10 * share * width, transcendentals=0
        ),
        name="pack",
    )(*blocks, rider)


def sums_kernel(last, weight_grad, gain_grad):
    width = weight_grad.shape[1]
    summed = last[0].astype(F32)
    for one in range(1, last.shape[0]):
        summed = summed + last[one].astype(F32)
    weight_grad[...] = summed[:, :width]
    extra = summed.shape[1] - width
    for row in range(summed.shape[0]):
        gain_grad[:, row * extra : (row + 1) * extra] = summed[row : row + 1, width:]


def last_sums(last, width):
    peers, rows, lanes = last.shape
    return pl.pallas_call(
        sums_kernel,
        out_shape=(
            jax.ShapeDtypeStruct((rows, width), F32),
            jax.ShapeDtypeStruct((1, rows * (lanes - width)), F32),
        ),
        in_specs=[pl.BlockSpec(memory_space=pltpu.VMEM)],
        out_specs=[pl.BlockSpec(memory_space=pltpu.VMEM)] * 2,
        compiler_params=pltpu.CompilerParams(vmem_limit_bytes=10 * 2**20),
        cost_estimate=pl.CostEstimate(
            flops=peers * rows * lanes, bytes_accessed=2 * peers * rows * lanes, transcendentals=0
        ),
        name="last_sums",
    )(last)


def rows_kernel(summands, gain, slices, rows):
    summed = [summands[i].astype(F32) for i in range(summands.shape[0])]
    dunit = ((summed[0] + summed[1]) + (summed[2] + summed[3])) * gain[...].astype(F32)
    resid_f = slices[0].astype(F32)
    inv = lax.rsqrt(jnp.mean(resid_f * resid_f, axis=-1, keepdims=True) + 1e-05)
    unit = resid_f * inv
    inner = jnp.mean(dunit * unit, axis=-1, keepdims=True)
    rows[...] = (slices[1].astype(F32) + inv * (dunit - unit * inner)).astype(BF16)


def result_rows(summands, gain, slices):
    _, rows, width = slices.shape
    return pl.pallas_call(
        rows_kernel,
        out_shape=jax.ShapeDtypeStruct((rows, width), BF16),
        in_specs=[pl.BlockSpec(memory_space=pltpu.VMEM)] * 3,
        out_specs=pl.BlockSpec(memory_space=pltpu.VMEM),
        compiler_params=pltpu.CompilerParams(vmem_limit_bytes=10 * 2**20),
        cost_estimate=pl.CostEstimate(
            flops=15 * rows * width, bytes_accessed=14 * rows * width, transcendentals=0
        ),
        name="result_rows",
    )(summands, gain, slices)


def body(resid, gain, grad_q, w_query, grad_in):
    tokens, width = resid.shape
    cols = grad_q.shape[1]
    core, zh = lax.axis_index("c"), lax.axis_index("zh")
    n_zh, n_x, n_y, n_zl = (lax.axis_size(a) for a in ("zh", "x", "y", "zl"))
    half = tokens // 2
    own = half // n_zh
    gain_f = gain.astype(F32)

    def rows_of(array, start, size):
        return lax.dynamic_slice_in_dim(array, start, size, 0)

    def inverse(rows):
        rows_f = rows.astype(F32)
        return lax.rsqrt(jnp.mean(rows_f * rows_f, axis=-1, keepdims=True) + 1e-05)

    def term(start):
        rows = rows_of(grad_q, start, half)
        return jnp.dot(rows, w_query, preferred_element_type=F32).astype(BF16)

    inv, grad_q = lax.optimization_barrier((inverse(resid), grad_q))

    other_start, own_start = (1 - core) * half, core * half
    sent = term(other_start)
    got = swapped(sent, "c", 1)
    kept = lax.optimization_barrier(term(own_start))
    pair = (kept.astype(F32) + got.astype(F32)).astype(BF16)
    held = (pair, inv, grad_q, resid, grad_in)
    pair, inv, grad_q, resid_x, grad_in = lax.optimization_barrier(held)
    summands = exchange(pair.reshape(n_zh, own, width), "zh")

    unit = resid.astype(F32) * inv
    part = jnp.sum(sent.astype(F32) * rows_of(unit, other_start, half), axis=0)
    part = part + jnp.sum(kept.astype(F32) * rows_of(unit, own_start, half), axis=0)
    part, inv_x = lax.optimization_barrier((part.reshape(-1, 128), inv))
    ordered = jnp.dot(grad_q, owner_columns(cols, lax.axis_index("x")), preferred_element_type=F32)
    ordered = lax.optimization_barrier(ordered.astype(BF16))
    part = part + swapped(part, "x", 1)
    part, inv_x = lax.optimization_barrier((part, inv_x))
    part_x = swapped(part, "x", 2)

    normed = (resid.astype(F32) * inv_x * gain_f).astype(BF16)
    share = cols // n_x

    def block(shift):
        columns = ordered[:, shift * share : (shift + 1) * share]
        local = lax.dot_general(
            columns, normed, (((0,), (0,)), ((), ())), preferred_element_type=F32
        )
        return lax.optimization_barrier(local.astype(BF16))

    blocks = [block(s) for s in range(n_x)]
    blocks = [b if s == 0 else shifted(b, "x", s) for s, b in enumerate(blocks)]
    first = own_start + zh * own
    slices = jnp.stack([rows_of(resid_x, first, own), rows_of(grad_in, first, own)])
    ready = (part + part_x, blocks[0], gain.reshape(1, width), slices)
    part, own_block, gain_row, slices = lax.optimization_barrier(ready)

    part, summands = lax.optimization_barrier((part, summands))
    part = jnp.broadcast_to(part[None], (lax.axis_size(TP), *part.shape))
    part = total(exchange(part, TP))
    rows = result_rows(summands, gain_row, slices)

    mine = share // (n_y * n_zl)
    packed = pack([own_block, *blocks[1:]], part.astype(BF16).reshape(mine, -1))
    last = exchange(packed, ("zl", "y"))
    weight_grad, gain_grad = last_sums(last, width)

    before, after = shifted(rows, "zh", 1), shifted(rows, "zh", n_zh - 1)
    upper, lower = before[: own // 2], after[own // 2 :]
    upper, lower = shifted(upper, "zh", 1), shifted(lower, "zh", n_zh - 1)
    result = jnp.zeros((tokens, width), BF16)
    for shift, piece in (
        (0, rows), (1, before), (n_zh - 1, after), (2, jnp.concatenate([upper, lower], axis=0))
    ):
        other = swapped(piece, "c", 1)
        source = lax.rem(zh + n_zh - shift, n_zh) * own
        result = lax.dynamic_update_slice_in_dim(result, piece, own_start + source, 0)
        result = lax.dynamic_update_slice_in_dim(result, other, other_start + source, 0)
    return weight_grad, gain_grad.reshape(-1), result


def solution(mesh):
    finer = Mesh(mesh.devices.reshape(3, 8, 4, 4, 2), ("zl", "y", "x", "zh", "c"))
    in_specs = (P(DP, None), P(), P(DP, TP), P(TP, None), P(DP, None))
    out_specs = (P(TP + DP, None), P(), P(DP, None))
    return jax.shard_map(body, mesh=finer, in_specs=in_specs, out_specs=out_specs, check_vma=False)
```
